256 devices in a mesh: seq: 128 (over y_lo, z, x, core), head: 2 (over y_hi).
Axes of the slice: x: 4, y: 4 (y_hi: 2, y_lo: 2; y = y_hi * 2 + y_lo), z: 8, core: 2. Of those that a mesh axis runs over, the one named last changes fastest.
Arguments:
- query: bfloat16 [65536, 1024], P('seq', 'head'), may hold values from -6 to 6
- key_rows: bfloat16 [65536, 128], P('seq'), may hold values from -6 to 6
- value_rows: bfloat16 [65536, 128], P('seq'), may hold values from -6 to 6
- output: bfloat16 [65536, 1024], P('seq', 'head'), may hold values from -1.5 to 1.5
- grad_output: bfloat16 [65536, 1024], P('seq', 'head'), may hold values from -144 to 144
- log_norm: float32 [8, 65536], P('head', 'seq'), may hold values from 0.5 to 12
- stripe: int32 [128], replicated, may hold values from 0 to 127, each once
Outputs:
- grad_query: bfloat16 [65536, 1024], P('seq', 'head')
- grad_key: bfloat16 [65536, 128], P(('seq', 'head'))
- grad_value: bfloat16 [65536, 128], P(('seq', 'head'))
The draws below stay inside these ranges and needn't reach their ends.
Inputs may be any that keep to these rules, and one draw needn't show every extreme that they name: stripe is a permutation of 0 to 127.
All inputs are finite; a program needn't handle non-finite values.
Results may differ from the reference program's by a relative error of at most 0.0051.
Values may be sent and summed in bfloat16 or wider, within the bound.
A program may use at most 192 MiB of HBM per device.

```python
import jax
import jax.numpy as jnp
from jax import lax

DH = 128
QH = 8
WINDOW = 8
S_DEV = 512
LEN = 65536
N_SEQ = 128


def draw_log_norm(key, part):
    local_row = (jnp.arange(LEN) % S_DEV).astype(jnp.float32)
    counts = WINDOW * (local_row + 0.5)
    base_level = jnp.log(counts) + 0.5
    jitter = jax.random.normal(key, (QH, LEN), jnp.float32) * 0.2
    return jnp.clip(base_level[None, :] + jitter, 0.5, 12.0).astype(jnp.float32)


def shard_levels(stream_key, shape, cuts, least, top_value):
    def one(position, parts):
        steps = jax.random.uniform(jax.random.fold_in(jax.random.fold_in(stream_key, 6), position), (parts,), jnp.float32, least / len(cuts), top_value / len(cuts))
        return jnp.repeat(jnp.exp(steps), shape[position] // parts).reshape((-1,) + (1,) * (len(shape) - position - 1))

    loudness = one(*cuts[0])
    for cut in cuts[1:]:
        loudness = loudness * one(*cut)
    return loudness


def scatter_about(rng, shape, deviation, bound, split=(), held_as=jnp.bfloat16):
    entries = jax.random.normal(rng, shape, jnp.float32) * deviation
    if len(split) > 0:
        entries = shard_levels(rng, shape, split, -0.22, 0.18) * entries
    return jnp.clip(entries, min=-bound, max=bound).astype(held_as)


def setup_inputs(seed: int = 0) -> dict:
    keys = jax.random.split(jax.random.key(seed), 8)
    query = scatter_about(keys[0], (LEN, QH * DH), 1.0, 6.0, ((0, 128), (1, 2)))
    key_rows = scatter_about(keys[1], (LEN, DH), 1.0, 6.0, ((0, 128),))
    value_rows = scatter_about(keys[2], (LEN, DH), 1.0, 6.0, ((0, 128),))
    output = scatter_about(keys[3], (LEN, QH * DH), 0.25, 1.5, ((0, 128), (1, 2)))
    grad_output = scatter_about(keys[4], (LEN, QH * DH), 24.0, 144.0, ((0, 128), (1, 2)))
    log_norm = draw_log_norm(jax.random.fold_in(keys[7], 71), 0)
    stripe = jax.random.permutation(keys[6], N_SEQ).astype(jnp.int32)
    return {"query": query, "key_rows": key_rows, "value_rows": value_rows, "output": output, "grad_output": grad_output, "log_norm": log_norm, "stripe": stripe}


def block_terms(query_heads, grad_heads, lse_rows, delta_rows, key_block, value_block, diag_open):
    extent = key_block.shape[0]
    factor = key_block.shape[1] ** -0.5
    scores = jnp.einsum("shd,td->hst", query_heads, key_block) * factor
    row_ids = lax.broadcasted_iota(jnp.int32, (extent, extent), 0)
    col_ids = lax.broadcasted_iota(jnp.int32, (extent, extent), 1)
    allowed = (col_ids < row_ids) | ((col_ids == row_ids) & diag_open)
    weights = jnp.where(allowed[None], jnp.exp(scores - lse_rows[:, :, None]), jnp.float32(0.0))
    weights_low = lax.optimization_barrier(weights.astype(jnp.bfloat16)).astype(jnp.float32)
    grad_values = jnp.einsum("hst,shd->td", weights_low, grad_heads)
    grad_weights = jnp.einsum("shd,td->hst", grad_heads, value_block)
    grad_scores = (factor * weights * (grad_weights - delta_rows[:, :, None])).astype(jnp.bfloat16)
    grad_scores = lax.optimization_barrier(grad_scores).astype(jnp.float32)
    grad_query = jnp.einsum("hst,td->shd", grad_scores, key_block)
    grad_keys = jnp.einsum("hst,shd->td", grad_scores, query_heads)
    return grad_query, jnp.stack([grad_keys, grad_values])


def reference(query, key_rows, value_rows, output, grad_output, log_norm, stripe):
    query_blocks = query.reshape(N_SEQ, S_DEV, QH, DH)
    grad_blocks = grad_output.reshape(N_SEQ, S_DEV, QH, DH)
    output_blocks = output.reshape(N_SEQ, S_DEV, QH, DH)
    lse_blocks = log_norm.reshape(QH, N_SEQ, S_DEV).transpose(1, 0, 2)
    key_blocks = key_rows.reshape(N_SEQ, S_DEV, DH)
    value_blocks = value_rows.reshape(N_SEQ, S_DEV, DH)

    def one_block(grad_kv, block_index):
        query_heads = query_blocks[block_index].astype(jnp.float32)
        grad_heads = grad_blocks[block_index].astype(jnp.float32)
        delta_rows = jnp.sum(grad_heads * output_blocks[block_index].astype(jnp.float32), axis=2).T
        lse_rows = lse_blocks[block_index]
        grad_query = jnp.zeros((S_DEV, QH, DH), jnp.float32)
        for offset in range(WINDOW):
            source = ((block_index - offset) % N_SEQ).astype(jnp.int32)
            diag_open = stripe[source] <= stripe[block_index]
            key_block = key_blocks[source].astype(jnp.float32)
            value_block = value_blocks[source].astype(jnp.float32)
            query_part, kv_part = block_terms(query_heads, grad_heads, lse_rows, delta_rows, key_block, value_block, diag_open)
            grad_query = grad_query + query_part
            grad_kv = grad_kv.at[source].add(kv_part)
        return grad_kv, grad_query.astype(jnp.bfloat16)

    start_kv = jnp.zeros((N_SEQ, 2, S_DEV, DH), jnp.float32)
    grad_kv, grad_query = lax.scan(one_block, start_kv, jnp.arange(N_SEQ, dtype=jnp.int32))
    grad_key = grad_kv[:, 0].reshape(LEN, DH).astype(jnp.bfloat16)
    grad_value = grad_kv[:, 1].reshape(LEN, DH).astype(jnp.bfloat16)
    return grad_query.reshape(LEN, QH * DH), grad_key, grad_value
```

```python
import functools
import math

import jax
import jax.numpy as jnp
from jax import lax
from jax.experimental import pallas as pl
from jax.experimental.pallas import tpu as pltpu
from jax.sharding import PartitionSpec as P

F32 = jnp.float32
BF16 = jnp.bfloat16
ROWS = 512
DH = 128
HEADS = 4
TILE = 128
TILES = ROWS // TILE
PAIR = 2 * TILE
UNITS = HEADS * ROWS // PAIR
HALF = ROWS // 2
LOG2E = math.log2(math.e)
SCALE = 1.0 / math.sqrt(DH)

OWN, E, PE, L, PL, PF, F, C = range(8)


def dot(a, b):
    return lax.dot_general(a, b, (((1,), (0,)), ((), ())), preferred_element_type=F32)


def lay_out(q_ref, o_ref, g_ref, lse_ref, q2, g2, qt, gt, lse2, delta):
    for h in range(HEADS):
        hp, e = divmod(h, 2)
        cols = slice(h * DH, (h + 1) * DH)
        q_h = q_ref[:, cols]
        g_h = g_ref[:, cols]
        q_t = q_h.T
        g_t = g_h.T
        sums = jnp.sum(g_t.astype(F32) * o_ref[:, cols].T.astype(F32), axis=0, keepdims=True)
        for j in range(TILES):
            u = hp * TILES + j
            at = u * PAIR + e * TILE
            rows = slice(j * TILE, (j + 1) * TILE)
            q2[at : at + TILE, :] = q_h[rows]
            g2[at : at + TILE, :] = g_h[rows]
            qt[:, at : at + TILE] = q_t[:, rows]
            gt[:, at : at + TILE] = g_t[:, rows]
            lse2[u : u + 1, e * TILE : (e + 1) * TILE] = lse_ref[h : h + 1, rows] * LOG2E
            delta[u : u + 1, e * TILE : (e + 1) * TILE] = sums[:, rows]


def pair_terms(k, v, qt, gt, lse2, delta, u, j, open_diag):
    depth = TILE * (j + 1)
    cols = slice(u * PAIR, (u + 1) * PAIR)
    scores = dot(k[0:depth, :], qt[:, cols])
    grad_p = dot(v[0:depth, :], gt[:, cols])
    p = jnp.exp2(scores * (LOG2E * SCALE) - lse2[u : u + 1, :])
    key_row = lax.broadcasted_iota(jnp.int32, (TILE, PAIR), 0)
    query_row = lax.broadcasted_iota(jnp.int32, (TILE, PAIR), 1) % TILE
    last = jnp.where(key_row < query_row + open_diag, p[depth - TILE :], 0.0)
    p = last if j == 0 else jnp.concatenate([p[: depth - TILE], last], 0)
    grad_s = ((p * SCALE) * (grad_p - delta[u : u + 1, :])).astype(BF16)
    return p.astype(BF16), grad_s


def block(kv, acc, open_diag, kt, q2, g2, qt, gt, lse2, delta, dqt):
    k, v = kv.at[0], kv.at[1]
    kt[...] = k[...].T
    for j in reversed(range(TILES)):
        depth = TILE * (j + 1)
        p0, s0 = pair_terms(k, v, qt, gt, lse2, delta, j, j, open_diag)
        p1, s1 = pair_terms(k, v, qt, gt, lse2, delta, TILES + j, j, open_diag)
        c0 = slice(j * PAIR, (j + 1) * PAIR)
        c1 = slice((TILES + j) * PAIR, (TILES + j + 1) * PAIR)
        grad_v = dot(p0, g2[c0, :]) + dot(p1, g2[c1, :])
        grad_k = dot(s0, q2[c0, :]) + dot(s1, q2[c1, :])
        if j == TILES - 1:
            acc[1, 0:depth, :] = grad_v
            acc[0, 0:depth, :] = grad_k
        else:
            acc[1, 0:depth, :] += grad_v
            acc[0, 0:depth, :] += grad_k
        dqt[:, c0] += dot(kt[:, 0:depth], s0)
        dqt[:, c1] += dot(kt[:, 0:depth], s1)


def kernel(
    n,
    stripe,
    q_hbm,
    k_hbm,
    v_hbm,
    o_hbm,
    g_hbm,
    lse_hbm,
    dq_hbm,
    dk_ref,
    dv_ref,
    q_ref,
    o_ref,
    g_ref,
    lse_ref,
    q2,
    g2,
    qt,
    gt,
    lse2,
    delta,
    kt,
    dqt,
    dq_ref,
    kvs,
    accs,
    p_out,
    p_in,
    y_out,
    y_in,
    x_out,
    d_out,
    r_in,
    load_sem,
    kv_send,
    kv_recv,
    p_send,
    p_recv,
    y_send,
    y_recv,
    x_send,
    d_send,
    r_recv,
    out_sem,
):
    me = lax.axis_index("seq")
    head = lax.axis_index("head")
    core = lax.rem(me, 2)

    def at(offset):
        return {"seq": lax.rem(me + offset + n, n), "head": head}

    partner = at(1 - 2 * core)
    across = {"seq": me, "head": 1 - head}

    loads = [
        pltpu.make_async_copy(k_hbm, kvs.at[OWN, 0], load_sem.at[0]),
        pltpu.make_async_copy(v_hbm, kvs.at[OWN, 1], load_sem.at[1]),
        pltpu.make_async_copy(q_hbm, q_ref, load_sem.at[2]),
        pltpu.make_async_copy(g_hbm, g_ref, load_sem.at[3]),
        pltpu.make_async_copy(o_hbm, o_ref, load_sem.at[4]),
        pltpu.make_async_copy(lse_hbm, lse_ref, load_sem.at[5]),
    ]
    for load in loads:
        load.start()

    barrier = pltpu.get_barrier_semaphore()
    peers = [partner, across, at(2), at(-2), at(6), at(-6), at(4), at(-4), at(14 * core - 7)]
    for peer in peers:
        pl.semaphore_signal(barrier, inc=1, device_id=peer, device_id_type=pl.DeviceIdType.MESH)

    def remote(src, dst, send, recv, to):
        return pltpu.make_async_remote_copy(
            src_ref=src, dst_ref=dst, send_sem=send, recv_sem=recv, device_id=to, device_id_type=pl.DeviceIdType.MESH
        )

    def pass_kv(src, dst, to):
        return remote(kvs.at[src], kvs.at[dst], kv_send.at[dst], kv_recv.at[dst], to)

    send_e = pass_kv(OWN, E, at(2 + 4 * core))
    send_l = pass_kv(OWN, L, at(6 - 4 * core))
    send_c = pass_kv(OWN, C, at(1 + 6 * core))
    pass_e = pass_kv(E, PE, partner)
    pass_on = pass_kv(E, F, at(2 - 4 * core))
    pass_l = pass_kv(L, PL, partner)
    pass_f = pass_kv(F, PF, partner)
    to_partner = [remote(p_out.at[m], p_in.at[m], p_send.at[m], p_recv.at[m], partner) for m in range(3)]
    exchange = [remote(y_out.at[m], y_in.at[m], y_send.at[m], y_recv.at[m], across) for m in range(3)]
    owners = [at(-2 - 4 * core), at(-6 + 4 * core), at(-4), at(-7 + 6 * core)]
    to_owner = [remote(x_out.at[m], r_in.at[m], x_send.at[m], r_recv.at[m], owners[m]) for m in range(2)]

    def both(m, o, into):
        far = {"seq": owners[o]["seq"], "head": 1 - head}
        return [
            remote(d_out.at[m], r_in.at[into], d_send.at[m], r_recv.at[into], owners[o]),
            remote(d_out.at[m + 1], r_in.at[into + 1], d_send.at[m + 1], r_recv.at[into + 1], far),
        ]

    direct = both(0, 2, 2) + both(2, 3, 4)

    mine = pl.ds(pl.multiple_of(head * HALF, HALF), HALF)
    other = pl.ds(pl.multiple_of((1 - head) * HALF, HALF), HALF)

    loads[0].wait()
    loads[1].wait()
    pl.semaphore_wait(barrier, len(peers))
    send_e.start()
    send_c.start()
    for load in loads[2:]:
        load.wait()
    lay_out(q_ref, o_ref, g_ref, lse_ref, q2, g2, qt, gt, lse2, delta)
    dqt[...] = jnp.zeros_like(dqt)
    own_stripe = stripe[me]
    back = [(0, 0), (2, 4), (5, -2), (6, -4), (1, 6), (3, 2), (4, 0), (7, -6)]

    def step(s, carry):
        behind = jnp.int32(0)
        for m in range(1, 8):
            behind = jnp.where(s == m, back[m][0] + back[m][1] * core, behind)

        @pl.when((s != OWN) & (s != F))
        def _():
            pltpu.make_async_copy(kvs.at[s], kvs.at[s], kv_recv.at[s]).wait()

        @pl.when(s == E)
        def _():
            pass_on.start()
            pass_e.start()

        @pl.when(s == L)
        def _():
            pass_l.start()

        @pl.when(s == PL)
        def _():
            pass_on.wait_recv()
            pass_f.start()

        source = lax.rem(me - behind + n, n)
        open_diag = jnp.where(stripe[source] <= own_stripe, 1, 0)
        block(kvs.at[s], accs.at[s], open_diag, kt, q2, g2, qt, gt, lse2, delta, dqt)

        @pl.when(s == OWN)
        def _():
            y_out[2] = accs[OWN, :, other, :].astype(BF16)
            exchange[2].start()
            send_e.wait_send()
            send_l.start()

        for m, (part, when) in enumerate(((PE, PE), (PL, PL), (PF, PF))):

            @pl.when(s == when)
            def _():
                p_out[m] = accs[part].astype(BF16)
                to_partner[m].start()

        for m, (part, when) in enumerate(((E, L), (L, PF))):

            @pl.when(s == when)
            def _():
                to_partner[m].wait_recv()
                y_out[m] = (accs[part, :, other, :] + p_in[m, :, other, :].astype(F32)).astype(BF16)
                exchange[m].start()

        def finish(m, part):
            exchange[m].wait_recv()
            total = accs[part, :, mine, :] + p_in[m, :, mine, :].astype(F32) + y_in[m].astype(F32)
            x_out[m] = total.astype(BF16)
            to_owner[m].start()

        @pl.when(s == F)
        def _():
            to_partner[2].wait_recv()
            d_out[1] = (accs[F, :, other, :] + p_in[2, :, other, :].astype(F32)).astype(BF16)
            direct[1].start()
            d_out[0] = (accs[F, :, mine, :] + p_in[2, :, mine, :].astype(F32)).astype(BF16)
            direct[0].start()
            finish(0, E)

        @pl.when(s == C)
        def _():
            d_out[3] = accs[C, :, other, :].astype(BF16)
            direct[3].start()
            d_out[2] = accs[C, :, mine, :].astype(BF16)
            direct[2].start()
            finish(1, L)

        return carry

    lax.fori_loop(0, 8, step, 0)

    for h in range(HEADS):
        hp, e = divmod(h, 2)
        for j in range(TILES):
            begin = (hp * TILES + j) * PAIR + e * TILE
            tile = dqt[:, begin : begin + TILE].astype(BF16).T
            dq_ref[j * TILE : (j + 1) * TILE, h * DH : (h + 1) * DH] = tile
    write = pltpu.make_async_copy(dq_ref, dq_hbm, out_sem)
    write.start()

    total = accs[OWN, :, mine, :]
    exchange[2].wait_recv()
    total = total + y_in[2].astype(F32)
    for copy in to_owner:
        copy.wait_recv()
    for copy in direct:
        copy.wait_recv()
    for m in range(6):
        total = total + r_in[m].astype(F32)
    dk_ref[...] = total[0].astype(BF16)
    dv_ref[...] = total[1].astype(BF16)
    for copy in [send_l, send_c, pass_e, pass_on, pass_l, pass_f] + to_partner + exchange + to_owner + direct:
        copy.wait_send()
    write.wait()


def solution(mesh):
    n = mesh.shape["seq"]
    half = (2, HALF, DH)

    def shards(query, key_rows, value_rows, output, grad_output, log_norm, stripe):
        anywhere = pl.BlockSpec(memory_space=pl.ANY)
        vmem = pl.BlockSpec(memory_space=pltpu.VMEM)
        dma = pltpu.SemaphoreType.DMA
        return pl.pallas_call(
            functools.partial(kernel, n),
            out_shape=(
                jax.ShapeDtypeStruct(query.shape, BF16),
                jax.ShapeDtypeStruct((HALF, DH), BF16),
                jax.ShapeDtypeStruct((HALF, DH), BF16),
            ),
            in_specs=[pl.BlockSpec(memory_space=pltpu.SMEM)] + [anywhere] * 6,
            out_specs=(anywhere, vmem, vmem),
            scratch_shapes=[
                pltpu.VMEM((ROWS, HEADS * DH), BF16),
                pltpu.VMEM((ROWS, HEADS * DH), BF16),
                pltpu.VMEM((ROWS, HEADS * DH), BF16),
                pltpu.VMEM((HEADS, ROWS), F32),
                pltpu.VMEM((UNITS * PAIR, DH), BF16),
                pltpu.VMEM((UNITS * PAIR, DH), BF16),
                pltpu.VMEM((DH, UNITS * PAIR), BF16),
                pltpu.VMEM((DH, UNITS * PAIR), BF16),
                pltpu.VMEM((UNITS, PAIR), F32),
                pltpu.VMEM((UNITS, PAIR), F32),
                pltpu.VMEM((DH, ROWS), BF16),
                pltpu.VMEM((DH, UNITS * PAIR), F32),
                pltpu.VMEM((ROWS, HEADS * DH), BF16),
                pltpu.VMEM((8, 2, ROWS, DH), BF16),
                pltpu.VMEM((8, 2, ROWS, DH), F32),
                pltpu.VMEM((3, 2, ROWS, DH), BF16),
                pltpu.VMEM((3, 2, ROWS, DH), BF16),
                pltpu.VMEM((3,) + half, BF16),
                pltpu.VMEM((3,) + half, BF16),
                pltpu.VMEM((2,) + half, BF16),
                pltpu.VMEM((4,) + half, BF16),
                pltpu.VMEM((6,) + half, BF16),
                dma((6,)),
                dma((8,)),
                dma((8,)),
                dma((3,)),
                dma((3,)),
                dma((3,)),
                dma((3,)),
                dma((2,)),
                dma((4,)),
                dma((6,)),
                dma,
            ],
            compiler_params=pltpu.CompilerParams(
                collective_id=0, has_side_effects=True, vmem_limit_bytes=60 * 2**20
            ),
            name="window_grads",
        )(stripe, query, key_rows, value_rows, output, grad_output, log_norm)

    placed = (
        P("seq", "head"),
        P("seq", None),
        P("seq", None),
        P("seq", "head"),
        P("seq", "head"),
        P("head", "seq"),
        P(),
    )
    return jax.shard_map(
        shards,
        mesh=mesh,
        in_specs=placed,
        out_specs=(P("seq", "head"), P(("seq", "head"), None), P(("seq", "head"), None)),
        check_vma=False,
    )
```

```python
import functools
import math

import jax
import jax.numpy as jnp
from jax import lax
from jax.experimental import pallas as pl
from jax.experimental.pallas import tpu as pltpu
from jax.sharding import PartitionSpec as P

F32 = jnp.float32
BF16 = jnp.bfloat16
ROWS = 512
DH = 128
HEADS = 4
TILE = 128
TILES = ROWS // TILE
WIDE = HEADS * TILE
HALF = ROWS // 2
LOG2E = math.log2(math.e)
SCALE = 1.0 / math.sqrt(DH)

OWN, E, PE, C, PF, F, PL, L = range(8)


def dot(a, b):
    return lax.dot_general(a, b, (((1,), (0,)), ((), ())), preferred_element_type=F32)


def lay_out(q_ref, o_ref, g_ref, lse_ref, q2, g2, qt, gt, lse2, delta):
    for h in range(HEADS):
        cols = slice(h * DH, (h + 1) * DH)
        q_h = q_ref[:, cols]
        g_h = g_ref[:, cols]
        q_t = q_h.T
        g_t = g_h.T
        sums = jnp.sum(g_t.astype(F32) * o_ref[:, cols].T.astype(F32), axis=0, keepdims=True)
        for j in range(TILES):
            at = j * WIDE + h * TILE
            rows = slice(j * TILE, (j + 1) * TILE)
            q2[at : at + TILE, :] = q_h[rows]
            g2[at : at + TILE, :] = g_h[rows]
            qt[:, at : at + TILE] = q_t[:, rows]
            gt[:, at : at + TILE] = g_t[:, rows]
            lse2[j : j + 1, h * TILE : (h + 1) * TILE] = lse_ref[h : h + 1, rows] * LOG2E
            delta[j : j + 1, h * TILE : (h + 1) * TILE] = sums[:, rows]


def half_block(part, kv, acc, open_diag, kt, q2, g2, qt, gt, lse2, delta, dqt):
    k, v = kv.at[0], kv.at[1]
    kt[...] = k[...].T
    first = True
    for j in reversed(range(2 * part, TILES)):
        rows = min(HALF, TILE * (j + 1) - HALF * part)
        cols = slice(j * WIDE, (j + 1) * WIDE)
        scores = dot(k[0:rows, :], qt[:, cols])
        grad_p = dot(v[0:rows, :], gt[:, cols])
        p = jnp.exp2(scores * (LOG2E * SCALE) - lse2[j : j + 1, :])
        if HALF * part + rows == TILE * (j + 1):
            key_row = lax.broadcasted_iota(jnp.int32, (TILE, WIDE), 0)
            query_row = lax.broadcasted_iota(jnp.int32, (TILE, WIDE), 1) % TILE
            last = jnp.where(key_row < query_row + open_diag, p[rows - TILE :], 0.0)
            p = last if rows == TILE else jnp.concatenate([p[: rows - TILE], last], 0)
        grad_s = ((p * SCALE) * (grad_p - delta[j : j + 1, :])).astype(BF16)
        grad_v = dot(p.astype(BF16), g2[cols, :])
        grad_k = dot(grad_s, q2[cols, :])
        if first:
            acc[1, 0:rows, :] = grad_v
            acc[0, 0:rows, :] = grad_k
        else:
            acc[1, 0:rows, :] += grad_v
            acc[0, 0:rows, :] += grad_k
        first = False
        dqt[:, cols] += dot(kt[:, 0:rows], grad_s)


def kernel(
    n,
    stripe,
    q_hbm,
    k_hbm,
    v_hbm,
    o_hbm,
    g_hbm,
    lse_hbm,
    dq_ref,
    dk_ref,
    dv_ref,
    q_ref,
    o_ref,
    g_ref,
    lse_ref,
    q2,
    g2,
    qt,
    gt,
    lse2,
    delta,
    kt,
    dqt,
    kvs,
    accs,
    p_out,
    p_in,
    r_out,
    own_out,
    r_in,
    load_sem,
    kv_send,
    kv_recv,
    p_send,
    p_recv,
    r_send,
    own_send,
    r_recv,
):
    me = lax.axis_index("seq")
    head = lax.axis_index("head")
    core = lax.rem(me, 2)

    def seq(offset):
        return lax.rem(me + offset + n, n)

    def at(offset):
        return {"seq": seq(offset), "head": head}

    partner = at(1 - 2 * core)
    across = {"seq": me, "head": 1 - head}

    loads = []
    for source, into in ((k_hbm, 0), (v_hbm, 1)):
        for part in range(2):
            rows = source.at[pl.ds(part * HALF, HALF)]
            loads.append(pltpu.make_async_copy(rows, kvs.at[OWN, part, into], load_sem.at[len(loads)]))
    for source, into in ((q_hbm, q_ref), (g_hbm, g_ref), (o_hbm, o_ref), (lse_hbm, lse_ref)):
        loads.append(pltpu.make_async_copy(source, into, load_sem.at[len(loads)]))
    for load in loads:
        load.start()

    barrier = pltpu.get_barrier_semaphore()
    peers = [partner, across, at(2), at(-2), at(6), at(-6), at(4), at(-4), at(14 * core - 7)]
    peers += [{"seq": peer["seq"], "head": 1 - head} for peer in [partner] + peers[2:]]
    for peer in peers:
        pl.semaphore_signal(barrier, inc=1, device_id=peer, device_id_type=pl.DeviceIdType.MESH)

    def remote(src, dst, send, recv, to):
        return pltpu.make_async_remote_copy(
            src_ref=src, dst_ref=dst, send_sem=send, recv_sem=recv, device_id=to, device_id_type=pl.DeviceIdType.MESH
        )

    def pass_kv(src, dst, to):
        return [
            remote(kvs.at[src, part], kvs.at[dst, part], kv_send.at[dst, part], kv_recv.at[dst, part], to)
            for part in range(2)
        ]

    send_e = pass_kv(OWN, E, at(2 + 4 * core))
    send_l = pass_kv(OWN, L, at(6 - 4 * core))
    send_c = pass_kv(OWN, C, at(1 + 6 * core))
    pass_e = pass_kv(E, PE, partner)
    pass_on = pass_kv(E, F, at(2 - 4 * core))
    pass_l = pass_kv(L, PL, partner)
    pass_f = pass_kv(F, PF, partner)
    to_partner = [
        [remote(p_out.at[m, part], p_in.at[m, part], p_send.at[m, part], p_recv.at[m, part], partner) for part in range(2)]
        for m in range(3)
    ]
    owners = [-2 - 4 * core, -6 + 4 * core, -4, -7 + 6 * core]

    def to_owner(m, part):
        slot = 2 * m + jnp.where(head == part, 0, 1)
        to = {"seq": seq(owners[m]), "head": part}
        return remote(r_out.at[m, part], r_in.at[slot], r_send.at[m, part], r_recv.at[slot], to)

    returns = [[to_owner(m, part) for part in range(2)] for m in range(4)]
    own_half = remote(own_out, r_in.at[8], own_send, r_recv.at[8], across)

    for load in loads[:4]:
        load.wait()
    pl.semaphore_wait(barrier, len(peers))
    for copy in send_e:
        copy.start()
    for load in loads[4:]:
        load.wait()
    lay_out(q_ref, o_ref, g_ref, lse_ref, q2, g2, qt, gt, lse2, delta)
    dqt[...] = jnp.zeros_like(dqt)
    own_stripe = stripe[me]
    back = {OWN: (0, 0), E: (2, 4), PE: (5, -2), C: (7, -6), PF: (3, 2), F: (4, 0), PL: (1, 6), L: (6, -4)}

    def relay(part):
        return [(E, send_e[part], [pass_on[part], pass_e[part]]), (C, pass_on[part], [pass_f[part]]), (F, send_l[part], [pass_l[part]])]

    def begin(s, part):
        @pl.when((s == PE) | (s == C) | (s == PF) | (s == PL))
        def _():
            pltpu.make_async_copy(kvs.at[s, part], kvs.at[s, part], kv_recv.at[s, part]).wait()

        for when, came, copies in relay(part):

            @pl.when(s == when)
            def _():
                came.wait_recv()
                for copy in copies:
                    copy.start()

    def send_back(m, block, part):
        total = accs[block, part]
        if m < 3:
            to_partner[m][part].wait_recv()
            total = total + p_in[m, part].astype(F32)
        r_out[m, part] = total.astype(BF16)
        returns[m][part].start()

    def finish(s, part):
        @pl.when((s == OWN) & (head != part))
        def _():
            own_out[...] = accs[OWN, part].astype(BF16)
            own_half.start()

        if part == 1:

            @pl.when(s == OWN)
            def _():
                for copy in send_c:
                    copy.start()

            @pl.when(s == E)
            def _():
                for copy in send_l:
                    copy.start()

        for m, block in enumerate((PE, PL, PF)):

            @pl.when(s == block)
            def _():
                p_out[m, part] = accs[block, part].astype(BF16)
                to_partner[m][part].start()

        @pl.when(s == C)
        def _():
            if part == 0:
                send_back(0, E, 0)
                send_back(0, E, 1)
            send_back(3, C, part)

        for m, block in ((2, F), (1, L)):

            @pl.when(s == block)
            def _():
                send_back(m, block, part)

    def step(s, carry):
        behind = jnp.int32(0)
        for block, (far, more) in back.items():
            behind = jnp.where(s == block, far + more * core, behind)
        open_diag = jnp.where(stripe[seq(-behind)] <= own_stripe, 1, 0)
        for part in range(2):
            begin(s, part)
            half_block(part, kvs.at[s, part], accs.at[s, part], open_diag, kt, q2, g2, qt, gt, lse2, delta, dqt)
            finish(s, part)
        return carry

    lax.fori_loop(0, 8, step, 0)

    for h in range(HEADS):
        for j in range(TILES):
            begin_col = j * WIDE + h * TILE
            tile = dqt[:, begin_col : begin_col + TILE].astype(BF16).T
            dq_ref[j * TILE : (j + 1) * TILE, h * DH : (h + 1) * DH] = tile

    total = accs[OWN, head]
    for slot in (6, 7, 8, 0, 1, 4, 5, 2, 3):
        pltpu.make_async_copy(r_in.at[slot], r_in.at[slot], r_recv.at[slot]).wait()
        total = total + r_in[slot].astype(F32)
    dk_ref[...] = total[0].astype(BF16)
    dv_ref[...] = total[1].astype(BF16)
    for copies in [send_e, send_l, send_c, pass_e, pass_on, pass_l, pass_f] + to_partner + returns + [[own_half]]:
        for copy in copies:
            copy.wait_send()


def solution(mesh):
    n = mesh.shape["seq"]
    half = (2, HALF, DH)

    def shards(query, key_rows, value_rows, output, grad_output, log_norm, stripe):
        anywhere = pl.BlockSpec(memory_space=pl.ANY)
        vmem = pl.BlockSpec(memory_space=pltpu.VMEM)
        dma = pltpu.SemaphoreType.DMA
        return pl.pallas_call(
            functools.partial(kernel, n),
            out_shape=(
                pltpu.VMEM(query.shape, BF16),
                pltpu.VMEM((HALF, DH), BF16),
                pltpu.VMEM((HALF, DH), BF16),
            ),
            in_specs=[pl.BlockSpec(memory_space=pltpu.SMEM)] + [anywhere] * 6,
            out_specs=(vmem, vmem, vmem),
            scratch_shapes=[
                pltpu.VMEM((ROWS, HEADS * DH), BF16),
                pltpu.VMEM((ROWS, HEADS * DH), BF16),
                pltpu.VMEM((ROWS, HEADS * DH), BF16),
                pltpu.VMEM((HEADS, ROWS), F32),
                pltpu.VMEM((TILES * WIDE, DH), BF16),
                pltpu.VMEM((TILES * WIDE, DH), BF16),
                pltpu.VMEM((DH, TILES * WIDE), BF16),
                pltpu.VMEM((DH, TILES * WIDE), BF16),
                pltpu.VMEM((TILES, WIDE), F32),
                pltpu.VMEM((TILES, WIDE), F32),
                pltpu.VMEM((DH, HALF), BF16),
                pltpu.VMEM((DH, TILES * WIDE), F32),
                pltpu.VMEM((8, 2) + half, BF16),
                pltpu.VMEM((8, 2) + half, F32),
                pltpu.VMEM((3, 2) + half, BF16),
                pltpu.VMEM((3, 2) + half, BF16),
                pltpu.VMEM((4, 2) + half, BF16),
                pltpu.VMEM(half, BF16),
                pltpu.VMEM((9,) + half, BF16),
                dma((8,)),
                dma((8, 2)),
                dma((8, 2)),
                dma((3, 2)),
                dma((3, 2)),
                dma((4, 2)),
                dma,
                dma((9,)),
            ],
            compiler_params=pltpu.CompilerParams(
                collective_id=0, has_side_effects=True, vmem_limit_bytes=60 * 2**20
            ),
            name="window_grads",
        )(stripe, query, key_rows, value_rows, output, grad_output, log_norm)

    placed = (
        P("seq", "head"),
        P("seq", None),
        P("seq", None),
        P("seq", "head"),
        P("seq", "head"),
        P("head", "seq"),
        P(),
    )
    return jax.shard_map(
        shards,
        mesh=mesh,
        in_specs=placed,
        out_specs=(P("seq", "head"), P(("seq", "head"), None), P(("seq", "head"), None)),
        check_vma=False,
    )
```

```python
import functools
import math

import jax
import jax.numpy as jnp
from jax import lax
from jax.experimental import pallas as pl
from jax.experimental.pallas import tpu as pltpu
from jax.sharding import PartitionSpec as P

F32 = jnp.float32
BF16 = jnp.bfloat16
ROWS = 512
DH = 128
HEADS = 4
TILE = 128
TILES = ROWS // TILE
WIDE = HEADS * TILE
HALF = ROWS // 2
LOG2E = math.log2(math.e)
SCALE = 1.0 / math.sqrt(DH)

OWN, E, PE, C, PF, F, PL, L = range(8)


def dot(a, b):
    return lax.dot_general(a, b, (((1,), (0,)), ((), ())), preferred_element_type=F32)


def lay_out(q_ref, o_ref, g_ref, lse_ref, q2, g2, qt, gt, lse2, delta):
    for h in range(HEADS):
        cols = slice(h * DH, (h + 1) * DH)
        q_h = q_ref[:, cols]
        g_h = g_ref[:, cols]
        q_t = q_h.T
        g_t = g_h.T
        sums = jnp.sum(g_t.astype(F32) * o_ref[:, cols].T.astype(F32), axis=0, keepdims=True)
        for j in range(TILES):
            at = j * WIDE + h * TILE
            rows = slice(j * TILE, (j + 1) * TILE)
            q2[at : at + TILE, :] = q_h[rows]
            g2[at : at + TILE, :] = g_h[rows]
            qt[:, at : at + TILE] = q_t[:, rows]
            gt[:, at : at + TILE] = g_t[:, rows]
            lse2[j : j + 1, h * TILE : (h + 1) * TILE] = lse_ref[h : h + 1, rows] * LOG2E
            delta[j : j + 1, h * TILE : (h + 1) * TILE] = sums[:, rows]


def half_block(part, kv, acc, open_diag, kt, q2, g2, qt, gt, lse2, delta, dqt):
    k, v = kv.at[0], kv.at[1]
    kt[...] = k[...].T
    first = True
    for j in reversed(range(2 * part, TILES)):
        rows = min(HALF, TILE * (j + 1) - HALF * part)
        cols = slice(j * WIDE, (j + 1) * WIDE)
        scores = dot(k[0:rows, :], qt[:, cols])
        grad_p = dot(v[0:rows, :], gt[:, cols])
        p = jnp.exp2(scores * (LOG2E * SCALE) - lse2[j : j + 1, :])
        if HALF * part + rows == TILE * (j + 1):
            key_row = lax.broadcasted_iota(jnp.int32, (TILE, WIDE), 0)
            query_row = lax.broadcasted_iota(jnp.int32, (TILE, WIDE), 1) % TILE
            last = jnp.where(key_row < query_row + open_diag, p[rows - TILE :], 0.0)
            p = last if rows == TILE else jnp.concatenate([p[: rows - TILE], last], 0)
        grad_s = ((p * SCALE) * (grad_p - delta[j : j + 1, :])).astype(BF16)
        grad_v = dot(p.astype(BF16), g2[cols, :])
        grad_k = dot(grad_s, q2[cols, :])
        if first:
            acc[1, 0:rows, :] = grad_v
            acc[0, 0:rows, :] = grad_k
        else:
            acc[1, 0:rows, :] += grad_v
            acc[0, 0:rows, :] += grad_k
        first = False
        dqt[:, cols] += dot(kt[:, 0:rows], grad_s)


def kernel(
    n,
    stripe,
    q_hbm,
    k_hbm,
    v_hbm,
    o_hbm,
    g_hbm,
    lse_hbm,
    dq_ref,
    dk_ref,
    dv_ref,
    q_ref,
    o_ref,
    g_ref,
    lse_ref,
    q2,
    g2,
    qt,
    gt,
    lse2,
    delta,
    kt,
    dqt,
    kvs,
    accs,
    p_out,
    p_in,
    r_out,
    own_out,
    f_in,
    r_in,
    load_sem,
    kv_send,
    kv_recv,
    p_send,
    p_recv,
    r_send,
    own_send,
    f_recv,
    r_recv,
):
    me = lax.axis_index("seq")
    head = lax.axis_index("head")
    core = lax.rem(me, 2)

    def seq(offset):
        return lax.rem(me + offset + n, n)

    def at(offset):
        return {"seq": seq(offset), "head": head}

    partner = at(1 - 2 * core)
    across = {"seq": me, "head": 1 - head}

    loads = []
    for source, into in ((k_hbm, 0), (v_hbm, 1)):
        for part in range(2):
            rows = source.at[pl.ds(part * HALF, HALF)]
            loads.append(pltpu.make_async_copy(rows, kvs.at[OWN, part, into], load_sem.at[len(loads)]))
    for source, into in ((q_hbm, q_ref), (g_hbm, g_ref), (o_hbm, o_ref), (lse_hbm, lse_ref)):
        loads.append(pltpu.make_async_copy(source, into, load_sem.at[len(loads)]))
    for load in loads:
        load.start()

    barrier = pltpu.get_barrier_semaphore()
    peers = [partner, across, at(2), at(-2), at(6), at(-6), at(4), at(-4), at(14 * core - 7)]
    peers += [{"seq": peer["seq"], "head": 1 - head} for peer in [partner] + peers[2:]]
    for peer in peers:
        pl.semaphore_signal(barrier, inc=1, device_id=peer, device_id_type=pl.DeviceIdType.MESH)

    def remote(src, dst, send, recv, to):
        return pltpu.make_async_remote_copy(
            src_ref=src, dst_ref=dst, send_sem=send, recv_sem=recv, device_id=to, device_id_type=pl.DeviceIdType.MESH
        )

    def pass_kv(src, dst, to):
        return [
            remote(kvs.at[src, part], kvs.at[dst, part], kv_send.at[dst, part], kv_recv.at[dst, part], to)
            for part in range(2)
        ]

    send_e = pass_kv(OWN, E, at(2 + 4 * core))
    send_l = pass_kv(OWN, L, at(6 - 4 * core))
    send_c = pass_kv(OWN, C, at(1 + 6 * core))
    pass_e = pass_kv(E, PE, partner)
    pass_on = pass_kv(E, F, at(2 - 4 * core))
    pass_l = pass_kv(L, PL, partner)
    pass_f = pass_kv(F, PF, partner)
    to_partner = [
        [remote(p_out.at[m, part], p_in.at[m, part], p_send.at[m, part], p_recv.at[m, part], partner) for part in range(2)]
        for m in range(3)
    ]
    owners = {0: -2 - 4 * core, 1: -6 + 4 * core, 3: -7 + 6 * core}
    first_slot = {0: 0, 1: 2, 3: 4}

    def to_owner(m, part):
        slot = first_slot[m] + jnp.where(head == part, 0, 1)
        to = {"seq": seq(owners[m]), "head": part}
        return remote(r_out.at[m, part], r_in.at[slot], r_send.at[m, part], r_recv.at[slot], to)

    returns = {m: [to_owner(m, part) for part in range(2)] for m in owners}
    returns[2] = [
        remote(r_out.at[2, part], f_in.at[part], r_send.at[2, part], f_recv.at[part], at(2 - 4 * core)) for part in range(2)
    ]
    own_half = remote(own_out, r_in.at[6], own_send, r_recv.at[6], across)

    for load in loads[:4]:
        load.wait()
    pl.semaphore_wait(barrier, len(peers))
    for copy in send_e:
        copy.start()
    for load in loads[4:]:
        load.wait()
    lay_out(q_ref, o_ref, g_ref, lse_ref, q2, g2, qt, gt, lse2, delta)
    dqt[...] = jnp.zeros_like(dqt)
    own_stripe = stripe[me]
    back = {OWN: (0, 0), E: (2, 4), PE: (5, -2), C: (7, -6), PF: (3, 2), F: (4, 0), PL: (1, 6), L: (6, -4)}

    def relay(part):
        return [(E, send_e[part], [pass_on[part], pass_e[part]]), (C, pass_on[part], [pass_f[part]]), (F, send_l[part], [pass_l[part]])]

    def begin(s, part):
        @pl.when((s == PE) | (s == C) | (s == PF) | (s == PL))
        def _():
            pltpu.make_async_copy(kvs.at[s, part], kvs.at[s, part], kv_recv.at[s, part]).wait()

        for when, came, copies in relay(part):

            @pl.when(s == when)
            def _():
                came.wait_recv()
                for copy in copies:
                    copy.start()

    def send_back(m, block, part):
        total = accs[block, part]
        if m < 3:
            to_partner[m][part].wait_recv()
            total = total + p_in[m, part].astype(F32)
        if m == 1:
            returns[2][part].wait_recv()
            total = total + f_in[part].astype(F32)
        r_out[m, part] = total.astype(BF16)
        returns[m][part].start()

    def finish(s, part):
        @pl.when((s == OWN) & (head != part))
        def _():
            own_out[...] = accs[OWN, part].astype(BF16)
            own_half.start()

        if part == 1:

            @pl.when(s == OWN)
            def _():
                for copy in send_c:
                    copy.start()

            @pl.when(s == E)
            def _():
                for copy in send_l:
                    copy.start()

        for m, block in enumerate((PE, PL, PF)):

            @pl.when(s == block)
            def _():
                p_out[m, part] = accs[block, part].astype(BF16)
                to_partner[m][part].start()

        @pl.when(s == C)
        def _():
            if part == 0:
                send_back(0, E, 0)
                send_back(0, E, 1)
            send_back(3, C, part)

        for m, block in ((2, F), (1, L)):

            @pl.when(s == block)
            def _():
                send_back(m, block, part)

    def step(s, carry):
        behind = jnp.int32(0)
        for block, (far, more) in back.items():
            behind = jnp.where(s == block, far + more * core, behind)
        open_diag = jnp.where(stripe[seq(-behind)] <= own_stripe, 1, 0)
        for part in range(2):
            begin(s, part)
            half_block(part, kvs.at[s, part], accs.at[s, part], open_diag, kt, q2, g2, qt, gt, lse2, delta, dqt)
            finish(s, part)
        return carry

    lax.fori_loop(0, 8, step, 0)

    for h in range(HEADS):
        for j in range(TILES):
            begin_col = j * WIDE + h * TILE
            tile = dqt[:, begin_col : begin_col + TILE].astype(BF16).T
            dq_ref[j * TILE : (j + 1) * TILE, h * DH : (h + 1) * DH] = tile

    total = accs[OWN, head]
    for slot in (4, 5, 6, 0, 1, 2, 3):
        pltpu.make_async_copy(r_in.at[slot], r_in.at[slot], r_recv.at[slot]).wait()
        total = total + r_in[slot].astype(F32)
    dk_ref[...] = total[0].astype(BF16)
    dv_ref[...] = total[1].astype(BF16)
    for copies in [send_e, send_l, send_c, pass_e, pass_on, pass_l, pass_f] + to_partner + list(returns.values()) + [[own_half]]:
        for copy in copies:
            copy.wait_send()


def solution(mesh):
    n = mesh.shape["seq"]
    half = (2, HALF, DH)

    def shards(query, key_rows, value_rows, output, grad_output, log_norm, stripe):
        anywhere = pl.BlockSpec(memory_space=pl.ANY)
        vmem = pl.BlockSpec(memory_space=pltpu.VMEM)
        dma = pltpu.SemaphoreType.DMA
        return pl.pallas_call(
            functools.partial(kernel, n),
            out_shape=(
                pltpu.VMEM(query.shape, BF16),
                pltpu.VMEM((HALF, DH), BF16),
                pltpu.VMEM((HALF, DH), BF16),
            ),
            in_specs=[pl.BlockSpec(memory_space=pltpu.SMEM)] + [anywhere] * 6,
            out_specs=(vmem, vmem, vmem),
            scratch_shapes=[
                pltpu.VMEM((ROWS, HEADS * DH), BF16),
                pltpu.VMEM((ROWS, HEADS * DH), BF16),
                pltpu.VMEM((ROWS, HEADS * DH), BF16),
                pltpu.VMEM((HEADS, ROWS), F32),
                pltpu.VMEM((TILES * WIDE, DH), BF16),
                pltpu.VMEM((TILES * WIDE, DH), BF16),
                pltpu.VMEM((DH, TILES * WIDE), BF16),
                pltpu.VMEM((DH, TILES * WIDE), BF16),
                pltpu.VMEM((TILES, WIDE), F32),
                pltpu.VMEM((TILES, WIDE), F32),
                pltpu.VMEM((DH, HALF), BF16),
                pltpu.VMEM((DH, TILES * WIDE), F32),
                pltpu.VMEM((8, 2) + half, BF16),
                pltpu.VMEM((8, 2) + half, F32),
                pltpu.VMEM((3, 2) + half, BF16),
                pltpu.VMEM((3, 2) + half, BF16),
                pltpu.VMEM((4, 2) + half, BF16),
                pltpu.VMEM(half, BF16),
                pltpu.VMEM((2,) + half, BF16),
                pltpu.VMEM((7,) + half, BF16),
                dma((8,)),
                dma((8, 2)),
                dma((8, 2)),
                dma((3, 2)),
                dma((3, 2)),
                dma((4, 2)),
                dma,
                dma((2,)),
                dma((7,)),
            ],
            compiler_params=pltpu.CompilerParams(
                collective_id=0, has_side_effects=True, vmem_limit_bytes=60 * 2**20
            ),
            name="window_grads",
        )(stripe, query, key_rows, value_rows, output, grad_output, log_norm)

    placed = (
        P("seq", "head"),
        P("seq", None),
        P("seq", None),
        P("seq", "head"),
        P("seq", "head"),
        P("head", "seq"),
        P(),
    )
    return jax.shard_map(
        shards,
        mesh=mesh,
        in_specs=placed,
        out_specs=(P("seq", "head"), P(("seq", "head"), None), P(("seq", "head"), None)),
        check_vma=False,
    )
```

```python
import functools
import math

import jax
import jax.numpy as jnp
from jax import lax
from jax.experimental import pallas as pl
from jax.experimental.pallas import tpu as pltpu
from jax.sharding import PartitionSpec as P

F32 = jnp.float32
BF16 = jnp.bfloat16
ROWS = 512
DH = 128
HEADS = 4
TILE = 128
TILES = ROWS // TILE
WIDE = HEADS * TILE
HALF = ROWS // 2
LOG2E = math.log2(math.e)
SCALE = 1.0 / math.sqrt(DH)

OWN, E, PE, C, PF, F, PL, L = range(8)


def dot(a, b):
    return lax.dot_general(a, b, (((1,), (0,)), ((), ())), preferred_element_type=F32)


def lay_out(q_ref, o_ref, g_ref, lse_ref, q2, g2, qt, gt, lse2, delta):
    for h in range(HEADS):
        cols = slice(h * DH, (h + 1) * DH)
        q_h = q_ref[:, cols]
        g_h = g_ref[:, cols]
        q_t = q_h.T
        g_t = g_h.T
        sums = jnp.sum(g_t.astype(F32) * o_ref[:, cols].T.astype(F32), axis=0, keepdims=True)
        for j in range(TILES):
            at = j * WIDE + h * TILE
            rows = slice(j * TILE, (j + 1) * TILE)
            q2[at : at + TILE, :] = q_h[rows]
            g2[at : at + TILE, :] = g_h[rows]
            qt[:, at : at + TILE] = q_t[:, rows]
            gt[:, at : at + TILE] = g_t[:, rows]
            lse2[j : j + 1, h * TILE : (h + 1) * TILE] = lse_ref[h : h + 1, rows] * LOG2E
            delta[j : j + 1, h * TILE : (h + 1) * TILE] = sums[:, rows]


def half_block(part, kv, acc, open_diag, kt, q2, g2, qt, gt, lse2, delta, dqt):
    k, v = kv.at[0], kv.at[1]
    kt[...] = k[...].T
    first = True
    for j in reversed(range(2 * part, TILES)):
        rows = min(HALF, TILE * (j + 1) - HALF * part)
        cols = slice(j * WIDE, (j + 1) * WIDE)
        scores = dot(k[0:rows, :], qt[:, cols])
        grad_p = dot(v[0:rows, :], gt[:, cols])
        p = jnp.exp2(scores * (LOG2E * SCALE) - lse2[j : j + 1, :])
        if HALF * part + rows == TILE * (j + 1):
            key_row = lax.broadcasted_iota(jnp.int32, (TILE, WIDE), 0)
            query_row = lax.broadcasted_iota(jnp.int32, (TILE, WIDE), 1) % TILE
            last = jnp.where(key_row < query_row + open_diag, p[rows - TILE :], 0.0)
            p = last if rows == TILE else jnp.concatenate([p[: rows - TILE], last], 0)
        grad_s = ((p * SCALE) * (grad_p - delta[j : j + 1, :])).astype(BF16)
        grad_v = dot(p.astype(BF16), g2[cols, :])
        grad_k = dot(grad_s, q2[cols, :])
        if first:
            acc[1, 0:rows, :] = grad_v
            acc[0, 0:rows, :] = grad_k
        else:
            acc[1, 0:rows, :] += grad_v
            acc[0, 0:rows, :] += grad_k
        first = False
        dqt[:, cols] += dot(kt[:, 0:rows], grad_s)


def kernel(
    n,
    stripe,
    q_hbm,
    k_hbm,
    v_hbm,
    o_hbm,
    g_hbm,
    lse_hbm,
    dq_ref,
    sums_ref,
    q_ref,
    o_ref,
    g_ref,
    lse_ref,
    q2,
    g2,
    qt,
    gt,
    lse2,
    delta,
    kt,
    dqt,
    kvs,
    accs,
    p_out,
    p_in,
    r_out,
    own_out,
    f_in,
    r_in,
    load_sem,
    kv_send,
    kv_recv,
    p_send,
    p_recv,
    r_send,
    own_send,
    f_recv,
    r_recv,
):
    me = lax.axis_index("seq")
    head = lax.axis_index("head")
    core = lax.rem(me, 2)

    def seq(offset):
        return lax.rem(me + offset + n, n)

    def at(offset):
        return {"seq": seq(offset), "head": head}

    partner = at(1 - 2 * core)
    across = {"seq": me, "head": 1 - head}

    loads = []
    for source, into in ((k_hbm, 0), (v_hbm, 1)):
        for part in range(2):
            rows = source.at[pl.ds(part * HALF, HALF)]
            loads.append(pltpu.make_async_copy(rows, kvs.at[OWN, part, into], load_sem.at[len(loads)]))
    for source, into in ((q_hbm, q_ref), (g_hbm, g_ref), (o_hbm, o_ref), (lse_hbm, lse_ref)):
        loads.append(pltpu.make_async_copy(source, into, load_sem.at[len(loads)]))
    for load in loads:
        load.start()

    barrier = pltpu.get_barrier_semaphore()
    came_from = [at(-2 - 4 * core), at(-6 + 4 * core), at(-2 + 4 * core), at(-7 + 6 * core)]
    read_by = [at(2 + 4 * core), at(6 - 4 * core), at(1 + 6 * core)]
    peers = [partner, across] + came_from + read_by
    peers += [{"seq": peer["seq"], "head": 1 - head} for peer in read_by]
    for peer in peers:
        pl.semaphore_signal(barrier, inc=1, device_id=peer, device_id_type=pl.DeviceIdType.MESH)

    def remote(src, dst, send, recv, to):
        return pltpu.make_async_remote_copy(
            src_ref=src, dst_ref=dst, send_sem=send, recv_sem=recv, device_id=to, device_id_type=pl.DeviceIdType.MESH
        )

    def pass_kv(src, dst, to):
        return [
            remote(kvs.at[src, part], kvs.at[dst, part], kv_send.at[dst, part], kv_recv.at[dst, part], to)
            for part in range(2)
        ]

    send_e = pass_kv(OWN, E, at(2 + 4 * core))
    send_l = pass_kv(OWN, L, at(6 - 4 * core))
    send_c = pass_kv(OWN, C, at(1 + 6 * core))
    pass_e = pass_kv(E, PE, partner)
    pass_on = pass_kv(E, F, at(2 - 4 * core))
    pass_l = pass_kv(L, PL, partner)
    pass_f = pass_kv(F, PF, partner)
    to_partner = [
        [remote(p_out.at[m, part], p_in.at[m, part], p_send.at[m, part], p_recv.at[m, part], partner) for part in range(2)]
        for m in range(3)
    ]
    owners = {0: -2 - 4 * core, 1: -6 + 4 * core, 3: -7 + 6 * core}
    first_slot = {0: 0, 1: 2, 3: 4}

    def to_owner(m, part):
        slot = first_slot[m] + jnp.where(head == part, 0, 1)
        to = {"seq": seq(owners[m]), "head": part}
        return remote(r_out.at[m, part], r_in.at[slot], r_send.at[m, part], r_recv.at[slot], to)

    returns = {m: [to_owner(m, part) for part in range(2)] for m in owners}
    returns[2] = [
        remote(r_out.at[2, part], f_in.at[part], r_send.at[2, part], f_recv.at[part], at(2 - 4 * core)) for part in range(2)
    ]
    own_half = remote(own_out, r_in.at[6], own_send, r_recv.at[6], across)

    for load in loads[:4]:
        load.wait()
    pl.semaphore_wait(barrier, len(peers))
    for copy in send_e:
        copy.start()
    for load in loads[4:]:
        load.wait()
    lay_out(q_ref, o_ref, g_ref, lse_ref, q2, g2, qt, gt, lse2, delta)
    dqt[...] = jnp.zeros_like(dqt)
    own_stripe = stripe[me]
    back = {OWN: (0, 0), E: (2, 4), PE: (5, -2), C: (7, -6), PF: (3, 2), F: (4, 0), PL: (1, 6), L: (6, -4)}

    def relay(part):
        return [(E, send_e[part], [pass_on[part], pass_e[part]]), (C, pass_on[part], [pass_f[part]]), (F, send_l[part], [pass_l[part]])]

    def begin(s, part):
        @pl.when((s == PE) | (s == C) | (s == PF) | (s == PL))
        def _():
            pltpu.make_async_copy(kvs.at[s, part], kvs.at[s, part], kv_recv.at[s, part]).wait()

        for when, came, copies in relay(part):

            @pl.when(s == when)
            def _():
                came.wait_recv()
                for copy in copies:
                    copy.start()

    def send_back(m, block, part):
        total = accs[block, part]
        if m < 3:
            to_partner[m][part].wait_recv()
            total = total + p_in[m, part].astype(F32)
        if m == 1:
            returns[2][part].wait_recv()
            total = total + f_in[part].astype(F32)
        r_out[m, part] = total.astype(BF16)
        returns[m][part].start()

    def finish(s, part):
        @pl.when((s == OWN) & (head != part))
        def _():
            own_out[...] = accs[OWN, part].astype(BF16)
            own_half.start()

        if part == 1:

            @pl.when(s == OWN)
            def _():
                for copy in send_c:
                    copy.start()

            @pl.when(s == E)
            def _():
                for copy in send_l:
                    copy.start()

        for m, block in enumerate((PE, PL, PF)):

            @pl.when(s == block)
            def _():
                p_out[m, part] = accs[block, part].astype(BF16)
                to_partner[m][part].start()

        @pl.when(s == C)
        def _():
            if part == 0:
                send_back(0, E, 0)
                send_back(0, E, 1)
            send_back(3, C, part)

        for m, block in ((2, F), (1, L)):

            @pl.when(s == block)
            def _():
                send_back(m, block, part)

    def step(s, carry):
        behind = jnp.int32(0)
        for block, (far, more) in back.items():
            behind = jnp.where(s == block, far + more * core, behind)
        open_diag = jnp.where(stripe[seq(-behind)] <= own_stripe, 1, 0)
        for part in range(2):
            begin(s, part)
            half_block(part, kvs.at[s, part], accs.at[s, part], open_diag, kt, q2, g2, qt, gt, lse2, delta, dqt)
            finish(s, part)
        return carry

    lax.fori_loop(0, 8, step, 0)

    for h in range(HEADS):
        for j in range(TILES):
            begin_col = j * WIDE + h * TILE
            tile = dqt[:, begin_col : begin_col + TILE].astype(BF16).T
            dq_ref[j * TILE : (j + 1) * TILE, h * DH : (h + 1) * DH] = tile

    total = accs[OWN, head]
    for slot in (4, 5, 6, 0, 1, 2, 3):
        pltpu.make_async_copy(r_in.at[slot], r_in.at[slot], r_recv.at[slot]).wait()
        total = total + r_in[slot].astype(F32)
    sums_ref[...] = total
    for copies in [send_e, send_l, send_c, pass_e, pass_on, pass_l, pass_f] + to_partner + list(returns.values()) + [[own_half]]:
        for copy in copies:
            copy.wait_send()


def solution(mesh):
    n = mesh.shape["seq"]
    half = (2, HALF, DH)

    def shards(query, key_rows, value_rows, output, grad_output, log_norm, stripe):
        anywhere = pl.BlockSpec(memory_space=pl.ANY)
        vmem = pl.BlockSpec(memory_space=pltpu.VMEM)
        dma = pltpu.SemaphoreType.DMA
        grad_query, sums = pl.pallas_call(
            functools.partial(kernel, n),
            out_shape=(
                pltpu.VMEM(query.shape, BF16),
                pltpu.VMEM(half, F32),
            ),
            in_specs=[pl.BlockSpec(memory_space=pltpu.SMEM)] + [anywhere] * 6,
            out_specs=(vmem, vmem),
            scratch_shapes=[
                pltpu.VMEM((ROWS, HEADS * DH), BF16),
                pltpu.VMEM((ROWS, HEADS * DH), BF16),
                pltpu.VMEM((ROWS, HEADS * DH), BF16),
                pltpu.VMEM((HEADS, ROWS), F32),
                pltpu.VMEM((TILES * WIDE, DH), BF16),
                pltpu.VMEM((TILES * WIDE, DH), BF16),
                pltpu.VMEM((DH, TILES * WIDE), BF16),
                pltpu.VMEM((DH, TILES * WIDE), BF16),
                pltpu.VMEM((TILES, WIDE), F32),
                pltpu.VMEM((TILES, WIDE), F32),
                pltpu.VMEM((DH, HALF), BF16),
                pltpu.VMEM((DH, TILES * WIDE), F32),
                pltpu.VMEM((8, 2) + half, BF16),
                pltpu.VMEM((8, 2) + half, F32),
                pltpu.VMEM((3, 2) + half, BF16),
                pltpu.VMEM((3, 2) + half, BF16),
                pltpu.VMEM((4, 2) + half, BF16),
                pltpu.VMEM(half, BF16),
                pltpu.VMEM((2,) + half, BF16),
                pltpu.VMEM((7,) + half, BF16),
                dma((8,)),
                dma((8, 2)),
                dma((8, 2)),
                dma((3, 2)),
                dma((3, 2)),
                dma((4, 2)),
                dma,
                dma((2,)),
                dma((7,)),
            ],
            compiler_params=pltpu.CompilerParams(
                collective_id=0, has_side_effects=True, vmem_limit_bytes=60 * 2**20
            ),
            name="window_grads",
        )(stripe, query, key_rows, value_rows, output, grad_output, log_norm)
        return grad_query, sums[0].astype(BF16), sums[1].astype(BF16)

    placed = (
        P("seq", "head"),
        P("seq", None),
        P("seq", None),
        P("seq", "head"),
        P("seq", "head"),
        P("head", "seq"),
        P(),
    )
    return jax.shard_map(
        shards,
        mesh=mesh,
        in_specs=placed,
        out_specs=(P("seq", "head"), P(("seq", "head"), None), P(("seq", "head"), None)),
        check_vma=False,
    )
```

```python
import functools
import math

import jax
import jax.numpy as jnp
from jax import lax
from jax.experimental import pallas as pl
from jax.experimental.pallas import tpu as pltpu
from jax.sharding import PartitionSpec as P

F32 = jnp.float32
BF16 = jnp.bfloat16
ROWS = 512
DH = 128
HEADS = 4
TILE = 128
TILES = ROWS // TILE
WIDE = HEADS * TILE
HALF = ROWS // 2
LOG2E = math.log2(math.e)
SCALE = 1.0 / math.sqrt(DH)

OWN, E, PE, C, PF, F, PL, L = range(8)


def dot(a, b):
    return lax.dot_general(a, b, (((1,), (0,)), ((), ())), preferred_element_type=F32)


def lay_out(q_ref, o_ref, g_ref, lse_ref, q2, g2, qt, gt, lse2, delta):
    for h in range(HEADS):
        cols = slice(h * DH, (h + 1) * DH)
        q_h = q_ref[:, cols]
        g_h = g_ref[:, cols]
        q_t = q_h.T
        g_t = g_h.T
        sums = jnp.sum(g_t.astype(F32) * o_ref[:, cols].T.astype(F32), axis=0, keepdims=True)
        for j in range(TILES):
            at = j * WIDE + h * TILE
            rows = slice(j * TILE, (j + 1) * TILE)
            q2[at : at + TILE, :] = q_h[rows]
            g2[at : at + TILE, :] = g_h[rows]
            qt[:, at : at + TILE] = q_t[:, rows]
            gt[:, at : at + TILE] = g_t[:, rows]
            lse2[j : j + 1, h * TILE : (h + 1) * TILE] = lse_ref[h : h + 1, rows] * LOG2E
            delta[j : j + 1, h * TILE : (h + 1) * TILE] = sums[:, rows]


def half_block(part, kv, acc, open_diag, kt, q2, g2, qt, gt, lse2, delta, dqt):
    k, v = kv.at[0], kv.at[1]
    kt[...] = k[...].T
    first = True
    for j in reversed(range(2 * part, TILES)):
        rows = min(HALF, TILE * (j + 1) - HALF * part)
        cols = slice(j * WIDE, (j + 1) * WIDE)
        scores = dot(k[0:rows, :], qt[:, cols])
        grad_p = dot(v[0:rows, :], gt[:, cols])
        p = jnp.exp2(scores * (LOG2E * SCALE) - lse2[j : j + 1, :])
        if HALF * part + rows == TILE * (j + 1):
            key_row = lax.broadcasted_iota(jnp.int32, (TILE, WIDE), 0)
            query_row = lax.broadcasted_iota(jnp.int32, (TILE, WIDE), 1) % TILE
            last = jnp.where(key_row < query_row + open_diag, p[rows - TILE :], 0.0)
            p = last if rows == TILE else jnp.concatenate([p[: rows - TILE], last], 0)
        grad_s = ((p * SCALE) * (grad_p - delta[j : j + 1, :])).astype(BF16)
        grad_v = dot(p.astype(BF16), g2[cols, :])
        grad_k = dot(grad_s, q2[cols, :])
        if first:
            acc[1, 0:rows, :] = grad_v
            acc[0, 0:rows, :] = grad_k
        else:
            acc[1, 0:rows, :] += grad_v
            acc[0, 0:rows, :] += grad_k
        first = False
        dqt[:, cols] += dot(kt[:, 0:rows], grad_s)


def kernel(
    n,
    stripe,
    q_hbm,
    k_hbm,
    v_hbm,
    o_hbm,
    g_hbm,
    lse_hbm,
    dq_ref,
    sums_ref,
    q_ref,
    o_ref,
    g_ref,
    lse_ref,
    q2,
    g2,
    qt,
    gt,
    lse2,
    delta,
    kt,
    dqt,
    kvs,
    accs,
    p_out,
    p_in,
    r_out,
    own_out,
    f_in,
    r_in,
    load_sem,
    kv_send,
    kv_recv,
    p_send,
    p_recv,
    r_send,
    own_send,
    f_recv,
    r_recv,
):
    me = lax.axis_index("seq")
    head = lax.axis_index("head")
    core = lax.rem(me, 2)

    def seq(offset):
        return lax.rem(me + offset + n, n)

    def at(offset):
        return {"seq": seq(offset), "head": head}

    partner = at(1 - 2 * core)
    across = {"seq": me, "head": 1 - head}

    loads = []
    for source, into in ((k_hbm, 0), (v_hbm, 1)):
        for part in range(2):
            rows = source.at[pl.ds(part * HALF, HALF)]
            loads.append(pltpu.make_async_copy(rows, kvs.at[OWN, part, into], load_sem.at[len(loads)]))
    for source, into in ((q_hbm, q_ref), (g_hbm, g_ref), (o_hbm, o_ref), (lse_hbm, lse_ref)):
        loads.append(pltpu.make_async_copy(source, into, load_sem.at[len(loads)]))
    for load in loads:
        load.start()

    barrier = pltpu.get_barrier_semaphore()
    came_from = [at(-2 - 4 * core), at(-6 + 4 * core), at(-2 + 4 * core), at(-7 + 6 * core)]
    read_by = [at(6 - 4 * core), at(1 + 6 * core)]
    peers = [partner, across] + came_from + read_by
    peers += [{"seq": peer["seq"], "head": 1 - head} for peer in read_by]
    for peer in peers:
        pl.semaphore_signal(barrier, inc=1, device_id=peer, device_id_type=pl.DeviceIdType.MESH)

    def remote(src, dst, send, recv, to):
        return pltpu.make_async_remote_copy(
            src_ref=src, dst_ref=dst, send_sem=send, recv_sem=recv, device_id=to, device_id_type=pl.DeviceIdType.MESH
        )

    def pass_kv(src, dst, to):
        return [
            remote(kvs.at[src, part], kvs.at[dst, part], kv_send.at[dst, part], kv_recv.at[dst, part], to)
            for part in range(2)
        ]

    send_e = pass_kv(OWN, E, at(2 + 4 * core))
    send_l = pass_kv(OWN, L, at(6 - 4 * core))
    send_c = pass_kv(OWN, C, at(1 + 6 * core))
    pass_e = pass_kv(E, PE, partner)
    pass_on = pass_kv(E, F, at(2 - 4 * core))
    pass_l = pass_kv(L, PL, partner)
    pass_f = pass_kv(F, PF, partner)
    to_partner = [
        [remote(p_out.at[m, part], p_in.at[m, part], p_send.at[m, part], p_recv.at[m, part], partner) for part in range(2)]
        for m in range(3)
    ]
    owners = {1: -6 + 4 * core, 3: -7 + 6 * core}
    first_slot = {1: 0, 3: 2}

    def to_owner(m, part):
        slot = first_slot[m] + jnp.where(head == part, 0, 1)
        to = {"seq": seq(owners[m]), "head": part}
        return remote(r_out.at[m, part], r_in.at[slot], r_send.at[m, part], r_recv.at[slot], to)

    returns = {m: [to_owner(m, part) for part in range(2)] for m in owners}
    for m in (0, 2):
        returns[m] = [
            remote(r_out.at[m, part], f_in.at[m // 2, part], r_send.at[m, part], f_recv.at[m // 2, part], at(2 - 4 * core))
            for part in range(2)
        ]
    own_half = remote(own_out, r_in.at[4], own_send, r_recv.at[4], across)

    for load in loads[:4]:
        load.wait()
    pl.semaphore_wait(barrier, len(peers))
    for copy in send_e:
        copy.start()
    for load in loads[4:]:
        load.wait()
    lay_out(q_ref, o_ref, g_ref, lse_ref, q2, g2, qt, gt, lse2, delta)
    dqt[...] = jnp.zeros_like(dqt)
    own_stripe = stripe[me]
    back = {OWN: (0, 0), E: (2, 4), PE: (5, -2), C: (7, -6), PF: (3, 2), F: (4, 0), PL: (1, 6), L: (6, -4)}

    def relay(part):
        return [(E, send_e[part], [pass_on[part], pass_e[part]]), (C, pass_on[part], [pass_f[part]]), (F, send_l[part], [pass_l[part]])]

    def begin(s, part):
        @pl.when((s == PE) | (s == C) | (s == PF) | (s == PL))
        def _():
            pltpu.make_async_copy(kvs.at[s, part], kvs.at[s, part], kv_recv.at[s, part]).wait()

        for when, came, copies in relay(part):

            @pl.when(s == when)
            def _():
                came.wait_recv()
                for copy in copies:
                    copy.start()

    def send_back(m, block, part):
        total = accs[block, part]
        if m < 3:
            to_partner[m][part].wait_recv()
            total = total + p_in[m, part].astype(F32)
        if m in (1, 2):
            returns[2 if m == 1 else 0][part].wait_recv()
            total = total + f_in[2 - m, part].astype(F32)
        r_out[m, part] = total.astype(BF16)
        returns[m][part].start()

    def finish(s, part):
        @pl.when((s == OWN) & (head != part))
        def _():
            own_out[...] = accs[OWN, part].astype(BF16)
            own_half.start()

        if part == 1:

            @pl.when(s == OWN)
            def _():
                for copy in send_c:
                    copy.start()

            @pl.when(s == E)
            def _():
                for copy in send_l:
                    copy.start()

        for m, block in enumerate((PE, PL, PF)):

            @pl.when(s == block)
            def _():
                p_out[m, part] = accs[block, part].astype(BF16)
                to_partner[m][part].start()

        @pl.when(s == C)
        def _():
            if part == 0:
                send_back(0, E, 0)
                send_back(0, E, 1)
            send_back(3, C, part)

        for m, block in ((2, F), (1, L)):

            @pl.when(s == block)
            def _():
                send_back(m, block, part)

    def step(s, carry):
        behind = jnp.int32(0)
        for block, (far, more) in back.items():
            behind = jnp.where(s == block, far + more * core, behind)
        open_diag = jnp.where(stripe[seq(-behind)] <= own_stripe, 1, 0)
        for part in range(2):
            begin(s, part)
            half_block(part, kvs.at[s, part], accs.at[s, part], open_diag, kt, q2, g2, qt, gt, lse2, delta, dqt)
            finish(s, part)
        return carry

    lax.fori_loop(0, 8, step, 0)

    for h in range(HEADS):
        for j in range(TILES):
            begin_col = j * WIDE + h * TILE
            tile = dqt[:, begin_col : begin_col + TILE].astype(BF16).T
            dq_ref[j * TILE : (j + 1) * TILE, h * DH : (h + 1) * DH] = tile

    total = accs[OWN, head]
    for slot in (2, 3, 4, 0, 1):
        pltpu.make_async_copy(r_in.at[slot], r_in.at[slot], r_recv.at[slot]).wait()
        total = total + r_in[slot].astype(F32)
    sums_ref[...] = total
    for copies in [send_e, send_l, send_c, pass_e, pass_on, pass_l, pass_f] + to_partner + list(returns.values()) + [[own_half]]:
        for copy in copies:
            copy.wait_send()


def solution(mesh):
    n = mesh.shape["seq"]
    half = (2, HALF, DH)

    def shards(query, key_rows, value_rows, output, grad_output, log_norm, stripe):
        anywhere = pl.BlockSpec(memory_space=pl.ANY)
        vmem = pl.BlockSpec(memory_space=pltpu.VMEM)
        dma = pltpu.SemaphoreType.DMA
        grad_query, sums = pl.pallas_call(
            functools.partial(kernel, n),
            out_shape=(
                pltpu.VMEM(query.shape, BF16),
                pltpu.VMEM(half, F32),
            ),
            in_specs=[pl.BlockSpec(memory_space=pltpu.SMEM)] + [anywhere] * 6,
            out_specs=(vmem, vmem),
            scratch_shapes=[
                pltpu.VMEM((ROWS, HEADS * DH), BF16),
                pltpu.VMEM((ROWS, HEADS * DH), BF16),
                pltpu.VMEM((ROWS, HEADS * DH), BF16),
                pltpu.VMEM((HEADS, ROWS), F32),
                pltpu.VMEM((TILES * WIDE, DH), BF16),
                pltpu.VMEM((TILES * WIDE, DH), BF16),
                pltpu.VMEM((DH, TILES * WIDE), BF16),
                pltpu.VMEM((DH, TILES * WIDE), BF16),
                pltpu.VMEM((TILES, WIDE), F32),
                pltpu.VMEM((TILES, WIDE), F32),
                pltpu.VMEM((DH, HALF), BF16),
                pltpu.VMEM((DH, TILES * WIDE), F32),
                pltpu.VMEM((8, 2) + half, BF16),
                pltpu.VMEM((8, 2) + half, F32),
                pltpu.VMEM((3, 2) + half, BF16),
                pltpu.VMEM((3, 2) + half, BF16),
                pltpu.VMEM((4, 2) + half, BF16),
                pltpu.VMEM(half, BF16),
                pltpu.VMEM((2, 2) + half, BF16),
                pltpu.VMEM((5,) + half, BF16),
                dma((8,)),
                dma((8, 2)),
                dma((8, 2)),
                dma((3, 2)),
                dma((3, 2)),
                dma((4, 2)),
                dma,
                dma((2, 2)),
                dma((5,)),
            ],
            compiler_params=pltpu.CompilerParams(
                collective_id=0, has_side_effects=True, vmem_limit_bytes=60 * 2**20
            ),
            name="window_grads",
        )(stripe, query, key_rows, value_rows, output, grad_output, log_norm)
        return grad_query, sums[0].astype(BF16), sums[1].astype(BF16)

    placed = (
        P("seq", "head"),
        P("seq", None),
        P("seq", None),
        P("seq", "head"),
        P("seq", "head"),
        P("head", "seq"),
        P(),
    )
    return jax.shard_map(
        shards,
        mesh=mesh,
        in_specs=placed,
        out_specs=(P("seq", "head"), P(("seq", "head"), None), P(("seq", "head"), None)),
        check_vma=False,
    )
```

```python
import functools
import math

import jax
import jax.numpy as jnp
from jax import lax
from jax.experimental import pallas as pl
from jax.experimental.pallas import tpu as pltpu
from jax.sharding import PartitionSpec as P

F32 = jnp.float32
BF16 = jnp.bfloat16
ROWS = 512
DH = 128
HEADS = 4
TILE = 128
TILES = ROWS // TILE
WIDE = HEADS * TILE
HALF = ROWS // 2
LOG2E = math.log2(math.e)
SCALE = 1.0 / math.sqrt(DH)

OWN, E, PE, C, PF, F, PL, L = range(8)


def dot(a, b):
    return lax.dot_general(a, b, (((1,), (0,)), ((), ())), preferred_element_type=F32)


def lay_out(q_ref, o_ref, g_ref, lse_ref, q2, g2, qt, gt, lse2, delta):
    for h in range(HEADS):
        cols = slice(h * DH, (h + 1) * DH)
        q_h = q_ref[:, cols]
        g_h = g_ref[:, cols]
        q_t = q_h.T
        g_t = g_h.T
        sums = jnp.sum(g_t.astype(F32) * o_ref[:, cols].T.astype(F32), axis=0, keepdims=True)
        for j in range(TILES):
            at = j * WIDE + h * TILE
            rows = slice(j * TILE, (j + 1) * TILE)
            q2[at : at + TILE, :] = q_h[rows]
            g2[at : at + TILE, :] = g_h[rows]
            qt[:, at : at + TILE] = q_t[:, rows]
            gt[:, at : at + TILE] = g_t[:, rows]
            lse2[j : j + 1, h * TILE : (h + 1) * TILE] = lse_ref[h : h + 1, rows] * LOG2E
            delta[j : j + 1, h * TILE : (h + 1) * TILE] = sums[:, rows]


def half_block(part, kv, acc, open_diag, kt, q2, g2, qt, gt, lse2, delta, dqt):
    k, v = kv.at[0], kv.at[1]
    kt[...] = k[...].T
    first = True
    for j in reversed(range(2 * part, TILES)):
        rows = min(HALF, TILE * (j + 1) - HALF * part)
        cols = slice(j * WIDE, (j + 1) * WIDE)
        scores = dot(k[0:rows, :], qt[:, cols])
        grad_p = dot(v[0:rows, :], gt[:, cols])
        p = jnp.exp2(scores * (LOG2E * SCALE) - lse2[j : j + 1, :])
        if HALF * part + rows == TILE * (j + 1):
            key_row = lax.broadcasted_iota(jnp.int32, (TILE, WIDE), 0)
            query_row = lax.broadcasted_iota(jnp.int32, (TILE, WIDE), 1) % TILE
            last = jnp.where(key_row < query_row + open_diag, p[rows - TILE :], 0.0)
            p = last if rows == TILE else jnp.concatenate([p[: rows - TILE], last], 0)
        grad_s = ((p * SCALE) * (grad_p - delta[j : j + 1, :])).astype(BF16)
        grad_v = dot(p.astype(BF16), g2[cols, :])
        grad_k = dot(grad_s, q2[cols, :])
        if first:
            acc[1, 0:rows, :] = grad_v
            acc[0, 0:rows, :] = grad_k
        else:
            acc[1, 0:rows, :] += grad_v
            acc[0, 0:rows, :] += grad_k
        first = False
        dqt[:, cols] += dot(kt[:, 0:rows], grad_s)


def kernel(
    n,
    stripe,
    q_hbm,
    k_hbm,
    v_hbm,
    o_hbm,
    g_hbm,
    lse_hbm,
    dq_ref,
    sums_ref,
    q_ref,
    o_ref,
    g_ref,
    lse_ref,
    q2,
    g2,
    qt,
    gt,
    lse2,
    delta,
    kt,
    dqt,
    kvs,
    accs,
    p_out,
    p_in,
    r_out,
    own_out,
    f_in,
    r_in,
    load_sem,
    kv_send,
    kv_recv,
    p_send,
    p_recv,
    r_send,
    own_send,
    f_recv,
    r_recv,
):
    me = lax.axis_index("seq")
    head = lax.axis_index("head")
    core = lax.rem(me, 2)

    def seq(offset):
        return lax.rem(me + offset + n, n)

    def at(offset):
        return {"seq": seq(offset), "head": head}

    partner = at(1 - 2 * core)
    across = {"seq": me, "head": 1 - head}

    loads = []
    for source, into in ((k_hbm, 0), (v_hbm, 1)):
        for part in range(2):
            rows = source.at[pl.ds(part * HALF, HALF)]
            loads.append(pltpu.make_async_copy(rows, kvs.at[OWN, part, into], load_sem.at[len(loads)]))
    for source, into in ((q_hbm, q_ref), (g_hbm, g_ref), (o_hbm, o_ref), (lse_hbm, lse_ref)):
        loads.append(pltpu.make_async_copy(source, into, load_sem.at[len(loads)]))
    for load in loads:
        load.start()

    barrier = pltpu.get_barrier_semaphore()
    came_from = [at(-2 - 4 * core), at(-6 + 4 * core), at(-2 + 4 * core), at(-7 + 6 * core)]
    read_by = [at(6 - 4 * core), at(1 + 6 * core)]
    peers = [partner, across] + came_from + read_by
    peers += [{"seq": peer["seq"], "head": 1 - head} for peer in read_by]
    for peer in peers:
        pl.semaphore_signal(barrier, inc=1, device_id=peer, device_id_type=pl.DeviceIdType.MESH)

    def remote(src, dst, send, recv, to):
        return pltpu.make_async_remote_copy(
            src_ref=src, dst_ref=dst, send_sem=send, recv_sem=recv, device_id=to, device_id_type=pl.DeviceIdType.MESH
        )

    def pass_kv(src, dst, to):
        return [
            remote(kvs.at[src, part], kvs.at[dst, part], kv_send.at[dst, part], kv_recv.at[dst, part], to)
            for part in range(2)
        ]

    send_e = pass_kv(OWN, E, at(2 + 4 * core))
    send_l = pass_kv(OWN, L, at(6 - 4 * core))
    send_c = pass_kv(OWN, C, at(1 + 6 * core))
    pass_e = pass_kv(E, PE, partner)
    pass_on = pass_kv(E, F, at(2 - 4 * core))
    pass_l = pass_kv(L, PL, partner)
    pass_f = pass_kv(F, PF, partner)
    to_partner = [
        [remote(p_out.at[m, part], p_in.at[m, part], p_send.at[m, part], p_recv.at[m, part], partner) for part in range(2)]
        for m in range(3)
    ]
    owners = {1: -6 + 4 * core, 3: -7 + 6 * core}
    first_slot = {1: 0, 3: 2}

    def to_owner(m, part):
        slot = first_slot[m] + jnp.where(head == part, 0, 1)
        to = {"seq": seq(owners[m]), "head": part}
        return remote(r_out.at[m, part], r_in.at[slot], r_send.at[m, part], r_recv.at[slot], to)

    returns = {m: [to_owner(m, part) for part in range(2)] for m in owners}
    for m in (0, 2):
        returns[m] = [
            remote(r_out.at[m, part], f_in.at[m // 2, part], r_send.at[m, part], f_recv.at[m // 2, part], at(2 - 4 * core))
            for part in range(2)
        ]
    own_half = remote(own_out, r_in.at[4], own_send, r_recv.at[4], across)

    for load in loads[:4]:
        load.wait()
    pl.semaphore_wait(barrier, len(peers))
    for copy in send_e:
        copy.start()
    for load in loads[4:]:
        load.wait()
    lay_out(q_ref, o_ref, g_ref, lse_ref, q2, g2, qt, gt, lse2, delta)
    dqt[...] = jnp.zeros_like(dqt)
    own_stripe = stripe[me]
    back = {OWN: (0, 0), E: (2, 4), PE: (5, -2), C: (7, -6), PF: (3, 2), F: (4, 0), PL: (1, 6), L: (6, -4)}

    def relay(part):
        return [(E, send_e[part], [pass_on[part], pass_e[part]]), (C, pass_on[part], [pass_f[part]]), (F, send_l[part], [pass_l[part]])]

    def begin(s, part):
        @pl.when((s == PE) | (s == C) | (s == PF) | (s == PL))
        def _():
            pltpu.make_async_copy(kvs.at[s, part], kvs.at[s, part], kv_recv.at[s, part]).wait()

        for when, came, copies in relay(part):

            @pl.when(s == when)
            def _():
                came.wait_recv()
                for copy in copies:
                    copy.start()

    def send_back(m, block, part):
        total = accs[block, part]
        if m < 3:
            to_partner[m][part].wait_recv()
            total = total + p_in[m, part].astype(F32)
        if m in (1, 2):
            returns[2 if m == 1 else 0][part].wait_recv()
            total = total + f_in[2 - m, part].astype(F32)
        r_out[m, part] = total.astype(BF16)
        returns[m][part].start()

    def finish(s, part):
        @pl.when((s == OWN) & (head != part))
        def _():
            own_out[...] = accs[OWN, part].astype(BF16)
            own_half.start()

        for when, copies in ((0, send_c), (1, send_l)):
            if part == when:

                @pl.when(s == E)
                def _():
                    for copy in copies:
                        copy.start()

        for m, block in enumerate((PE, PL, PF)):

            @pl.when(s == block)
            def _():
                p_out[m, part] = accs[block, part].astype(BF16)
                to_partner[m][part].start()

        @pl.when(s == C)
        def _():
            if part == 0:
                send_back(0, E, 0)
                send_back(0, E, 1)
            send_back(3, C, part)

        for m, block in ((2, F), (1, L)):

            @pl.when(s == block)
            def _():
                send_back(m, block, part)

    def step(s, carry):
        behind = jnp.int32(0)
        for block, (far, more) in back.items():
            behind = jnp.where(s == block, far + more * core, behind)
        open_diag = jnp.where(stripe[seq(-behind)] <= own_stripe, 1, 0)
        for part in range(2):
            begin(s, part)
            half_block(part, kvs.at[s, part], accs.at[s, part], open_diag, kt, q2, g2, qt, gt, lse2, delta, dqt)
            finish(s, part)
        return carry

    lax.fori_loop(0, 8, step, 0)

    for h in range(HEADS):
        for j in range(TILES):
            begin_col = j * WIDE + h * TILE
            tile = dqt[:, begin_col : begin_col + TILE].astype(BF16).T
            dq_ref[j * TILE : (j + 1) * TILE, h * DH : (h + 1) * DH] = tile

    total = accs[OWN, head]
    for slot in (2, 3, 4, 0, 1):
        pltpu.make_async_copy(r_in.at[slot], r_in.at[slot], r_recv.at[slot]).wait()
        total = total + r_in[slot].astype(F32)
    sums_ref[...] = total
    for copies in [send_e, send_l, send_c, pass_e, pass_on, pass_l, pass_f] + to_partner + list(returns.values()) + [[own_half]]:
        for copy in copies:
            copy.wait_send()


def solution(mesh):
    n = mesh.shape["seq"]
    half = (2, HALF, DH)

    def shards(query, key_rows, value_rows, output, grad_output, log_norm, stripe):
        anywhere = pl.BlockSpec(memory_space=pl.ANY)
        vmem = pl.BlockSpec(memory_space=pltpu.VMEM)
        dma = pltpu.SemaphoreType.DMA
        grad_query, sums = pl.pallas_call(
            functools.partial(kernel, n),
            out_shape=(
                pltpu.VMEM(query.shape, BF16),
                pltpu.VMEM(half, F32),
            ),
            in_specs=[pl.BlockSpec(memory_space=pltpu.SMEM)] + [anywhere] * 6,
            out_specs=(vmem, vmem),
            scratch_shapes=[
                pltpu.VMEM((ROWS, HEADS * DH), BF16),
                pltpu.VMEM((ROWS, HEADS * DH), BF16),
                pltpu.VMEM((ROWS, HEADS * DH), BF16),
                pltpu.VMEM((HEADS, ROWS), F32),
                pltpu.VMEM((TILES * WIDE, DH), BF16),
                pltpu.VMEM((TILES * WIDE, DH), BF16),
                pltpu.VMEM((DH, TILES * WIDE), BF16),
                pltpu.VMEM((DH, TILES * WIDE), BF16),
                pltpu.VMEM((TILES, WIDE), F32),
                pltpu.VMEM((TILES, WIDE), F32),
                pltpu.VMEM((DH, HALF), BF16),
                pltpu.VMEM((DH, TILES * WIDE), F32),
                pltpu.VMEM((8, 2) + half, BF16),
                pltpu.VMEM((8, 2) + half, F32),
                pltpu.VMEM((3, 2) + half, BF16),
                pltpu.VMEM((3, 2) + half, BF16),
                pltpu.VMEM((4, 2) + half, BF16),
                pltpu.VMEM(half, BF16),
                pltpu.VMEM((2, 2) + half, BF16),
                pltpu.VMEM((5,) + half, BF16),
                dma((8,)),
                dma((8, 2)),
                dma((8, 2)),
                dma((3, 2)),
                dma((3, 2)),
                dma((4, 2)),
                dma,
                dma((2, 2)),
                dma((5,)),
            ],
            compiler_params=pltpu.CompilerParams(
                collective_id=0, has_side_effects=True, vmem_limit_bytes=60 * 2**20
            ),
            name="window_grads",
        )(stripe, query, key_rows, value_rows, output, grad_output, log_norm)
        return grad_query, sums[0].astype(BF16), sums[1].astype(BF16)

    placed = (
        P("seq", "head"),
        P("seq", None),
        P("seq", None),
        P("seq", "head"),
        P("seq", "head"),
        P("head", "seq"),
        P(),
    )
    return jax.shard_map(
        shards,
        mesh=mesh,
        in_specs=placed,
        out_specs=(P("seq", "head"), P(("seq", "head"), None), P(("seq", "head"), None)),
        check_vma=False,
    )
```
